256 devices in a mesh: tm: 8 (over z), par: 32 (over x, y, core).
Axes of the slice: x: 4, y: 4, z: 8, core: 2. Of those that a mesh axis runs over, the one named last changes fastest.
Arguments:
- kernel: bfloat16 [128, 256, 4096], P('tm', None, 'par'), may hold values from -0.015625 to 0.015625
- history: bfloat16 [128, 4096, 128], P('tm', 'par'), may hold values from -6 to 6
- arrivals: bfloat16 [2, 16, 4096, 128], P(None, 'tm', 'par'), may hold values from -6 to 6
Outputs:
- observations: bfloat16 [2, 16, 256, 128], P(None, None, ('tm', 'par'))
The draws below stay inside these ranges and needn't reach their ends.
All inputs are finite; a program needn't handle non-finite values.
Results may differ from the reference program's by a relative error of at most 0.014.
Values may be sent and summed in bfloat16 or wider, within the bound.
A program may use at most 64 MiB of HBM per device.

```python
import jax
import jax.numpy as jnp
from jax import lax

TB = 16
NF = 17
SENS = 256
FIELDS = 128
STEPS = 2
NT = 128
NP = 4096
N_TM = 8


def strengthened(entries, stream_key, source, target, shards_of, factor):
    owner, partner = [(jnp.arange(entries.shape[axis_at]) // (entries.shape[axis_at] // shards_of)).reshape([-1 if axis == axis_at else 1 for axis in range(entries.ndim)]) for axis_at in (source, target)]
    chosen = jax.random.permutation(stream_key, shards_of)[partner]
    strong = (owner == chosen) | (owner == (partner + shards_of // 2) % shards_of)
    return jnp.where(strong, factor * entries, entries)


def levels(own_key, dims, cuts, least, top_value):
    def one(position, parts):
        draws = jax.random.uniform(jax.random.fold_in(jax.random.fold_in(own_key, 6), position), (parts,), jnp.float32, least / len(cuts), top_value / len(cuts))
        return jnp.repeat(jnp.exp(draws), dims[position] // parts).reshape((-1,) + (1,) * (len(dims) - position - 1))

    gain = one(*cuts[0])
    for cut in cuts[1:]:
        gain = gain * one(*cut)
    return gain


def normal_values(rng, shape, scale, limit, cuts=(), kind=jnp.bfloat16):
    loudness = levels(rng, shape, cuts, -0.22, 0.18) if cuts else 1.0
    result = jax.random.normal(rng, shape, jnp.float32) * scale * loudness
    return jnp.minimum(jnp.maximum(result, -limit), limit).astype(kind)


def noise_with(key, shape, spread, reach, shards, heavy, kind=jnp.bfloat16):
    drawn = spread * jax.random.normal(key, shape, jnp.float32)
    if shards:
        drawn = drawn * levels(key, shape, shards, -0.22, 0.18)
    return jnp.clip(strengthened(drawn, jax.random.fold_in(key, 3), *heavy), -reach, reach).astype(kind)


def setup_inputs(seed: int = 0) -> dict:
    streams_of = jax.random.split(jax.random.key(seed), 4)
    return {
        "kernel": noise_with(streams_of[0], (NT, SENS, NP), (NT * NP) ** -0.5, 0.015625, ((0, 8), (2, 32)), (2, 1, 32, 2.75)),
        "history": normal_values(streams_of[1], (NT, NP, FIELDS), 1.0, 6.0, ((0, 8), (1, 32))),
        "arrivals": normal_values(streams_of[2], (STEPS, TB, NP, FIELDS), 1.0, 6.0, ((1, 8), (2, 32))),
    }


def rounded(values):
    narrow = values.astype(jnp.bfloat16)
    narrow = lax.optimization_barrier(narrow)
    return narrow.astype(jnp.float32)


def reference(kernel, history, arrivals):
    length = 2 * TB
    ordered = jnp.concatenate([history.reshape(N_TM, TB, NP, FIELDS)[::-1], arrivals], 0)
    accum_shape = (STEPS, NF, SENS, FIELDS)

    def one_lag(totals, lag_index):
        real_acc, imag_acc = totals
        first_row = (lag_index * TB).astype(jnp.int32)
        lag_block = lax.dynamic_slice_in_dim(kernel, first_row, TB, 0).astype(jnp.float32)
        spectrum = jnp.fft.rfft(lag_block, n=length, axis=0)
        kernel_real_component = rounded(jnp.real(spectrum))
        kernel_imaginary = rounded(jnp.imag(spectrum))
        for step_index in range(STEPS):
            first_block = (N_TM - 1 + step_index - lag_index).astype(jnp.int32)
            window = lax.dynamic_slice_in_dim(ordered, first_block, 2, 0)
            window = window.reshape(length, NP, FIELDS).astype(jnp.float32)
            window_spec = jnp.fft.rfft(window, axis=0)
            window_real_component = rounded(jnp.real(window_spec))
            window_imaginary = rounded(jnp.imag(window_spec))
            real_component = jnp.einsum("njy,nyv->njv", kernel_real_component, window_real_component, precision=lax.Precision.HIGHEST)
            real_component = real_component - jnp.einsum("njy,nyv->njv", kernel_imaginary, window_imaginary, precision=lax.Precision.HIGHEST)
            imaginary_component = jnp.einsum("njy,nyv->njv", kernel_real_component, window_imaginary, precision=lax.Precision.HIGHEST)
            imaginary_component = imaginary_component + jnp.einsum("njy,nyv->njv", kernel_imaginary, window_real_component, precision=lax.Precision.HIGHEST)
            real_acc = real_acc.at[step_index].add(real_component)
            imag_acc = imag_acc.at[step_index].add(imaginary_component)
        return (real_acc, imag_acc), None

    zeros_start = jnp.zeros(accum_shape, jnp.float32)
    (real_acc, imag_acc), unused = lax.scan(one_lag, (zeros_start, zeros_start), jnp.arange(N_TM, dtype=jnp.int32))
    signal = jnp.fft.irfft(lax.complex(real_acc, imag_acc), n=length, axis=1)
    return signal[:, TB:].astype(jnp.bfloat16)
```

```python
import jax
import jax.numpy as jnp
from jax import lax
from jax.experimental import pallas as pl
from jax.experimental.pallas import tpu as pltpu
from jax.sharding import Mesh
from jax.sharding import PartitionSpec as P

PAR = ("px", "py", "pc")
MESH = pl.DeviceIdType.MESH
CHUNK = 4
PIECE = 2


def kernel(k_hbm, h_hbm, a_hbm, out_ref, kv, krev, w, w2, relay, d2s, d2o, d2r, s1, o1, r1, s2, o2, r2, yb, zs, zo, zr,
           local_sem, w_recv, own_send, fwd_send, arr_send, relay_recv, relay_send, d2_send, d2_recv,
           s1_send, s1_recv, s2_send, s2_recv, z_send, z_recv):
    z, x, y, c = (lax.axis_index(name) for name in ("tm", "px", "py", "pc"))
    nz, nx, ny, nc = 8, 4, 4, 2
    steps = 32
    chunks = steps // CHUNK
    lanes = CHUNK * 128
    sizes = {"tm": nz, "px": nx, "py": ny, "pc": nc}
    here = {"tm": z, "px": x, "py": y, "pc": c}

    def ahead(name, by):
        return {name: lax.rem(here[name] + by, sizes[name])}

    copy_k = pltpu.make_async_copy(k_hbm, kv, local_sem.at[0])
    copy_k.start()
    copy_h = pltpu.make_async_copy(h_hbm, w.at[pl.ds(0, 16)], local_sem.at[1])
    copy_h.start()

    barrier = pltpu.get_barrier_semaphore()
    peers = [(name, by) for name in sizes for by in range(1, sizes[name])]
    for name, by in peers:
        pl.semaphore_signal(barrier, inc=1, device_id=ahead(name, by), device_id_type=MESH)
    pl.semaphore_wait(barrier, len(peers))

    def remote(src, dst, send_sem, recv_sem, target):
        return pltpu.make_async_remote_copy(
            src_ref=src, dst_ref=dst, send_sem=send_sem, recv_sem=recv_sem, device_id=target, device_id_type=MESH
        )

    def own_piece(i):
        return remote(h_hbm.at[pl.ds(2 * i, 2)], w.at[pl.ds(16 + 2 * i, 2)], own_send.at[i], w_recv.at[0, i], ahead("tm", 1))

    def forward_piece(i):
        return remote(
            w.at[pl.ds(16 + 2 * i, 2)], w.at[pl.ds(32 + 2 * i, 2)], fwd_send.at[i], w_recv.at[1, i], ahead("tm", 1)
        )

    def wait_piece(blk, i):
        ref = w.at[pl.ds(16 + 16 * blk + 2 * i, 2)]
        remote(ref, ref, fwd_send.at[i], w_recv.at[blk, i], ahead("tm", 1)).wait_recv()

    def arrival_piece(s, owner):
        return remote(
            a_hbm.at[s], w.at[pl.ds(16 + 16 * s + 2 * owner, 2)], arr_send.at[s], w_recv.at[s, owner], {"tm": 0}
        )

    def to_relay(s):
        return remote(a_hbm.at[s], relay.at[s], arr_send.at[s], relay_recv.at[s], ahead("tm", nz - 3))

    def from_relay(s, owner):
        return remote(
            relay.at[s], w.at[pl.ds(16 + 16 * s + 2 * owner, 2)], relay_send.at[s], w_recv.at[s, owner], {"tm": 0}
        )

    def local_arrival(s):
        return pltpu.make_async_copy(a_hbm.at[s], w.at[pl.ds(16 + 16 * s, 2)], w_recv.at[s, 0])

    @pl.when(z == 0)
    def _():
        for s in range(2):
            local_arrival(s).start()

    @pl.when(z < nz - 1)
    def _():
        for i in range(8):
            own_piece(i).start()

    for s in range(2):
        for owner in (1, 2, 3, 7):

            @pl.when(z == owner)
            def _():
                arrival_piece(s, owner).start()

        @pl.when((z >= 4) & (z <= 6))
        def _():
            to_relay(s).start()

    row = lax.broadcasted_iota(jnp.int32, (256, 256), 0)
    col = lax.broadcasted_iota(jnp.int32, (256, 256), 1)
    core_of = (c + (row >> 7)) & 1
    x_of = (x + (row >> 5)) & 3
    y_of = (y + (row >> 3)) & 3
    z_of = (z + row) & 7
    sensor = z_of * 32 + x_of * 8 + y_of * 2 + core_of
    order = jnp.where(sensor == col, 1.0, 0.0).astype(jnp.bfloat16)
    copy_k.wait()
    for lag in range(16):
        moved = jnp.dot(order, kv[lag], preferred_element_type=jnp.float32)
        krev[:, (15 - lag) * 128 : (16 - lag) * 128] = moved.astype(jnp.bfloat16)

    def place(t):
        block = w[t]
        w2[t * 128 : (t + 1) * 128, 0:128] = block
        if t > 0:
            w2[(t - 1) * 128 : t * 128, 128:256] = block

    copy_h.wait()
    for t in range(16):
        place(t)

    def order_of(g):
        return ("px", "py") if g % 2 == 0 else ("py", "px")

    def core_copy(g):
        return remote(d2s.at[g], d2r.at[g], d2_send.at[g], d2_recv.at[g], ahead("pc", 1))

    def first_copy(g, d):
        return remote(
            s1.at[g, d - 1], r1.at[g, d - 1], s1_send.at[g, d - 1], s1_recv.at[g, d - 1], ahead(order_of(g)[0], d)
        )

    def second_copy(g, d):
        return remote(
            s2.at[g, d - 1], r2.at[g, d - 1], s2_send.at[g, d - 1], s2_recv.at[g, d - 1], ahead(order_of(g)[1], d)
        )

    def z_copy(s, d):
        return remote(zs.at[s, d - 1], zr.at[s, d - 1], z_send.at[s, d - 1], z_recv.at[s, d - 1], ahead("tm", d))

    def compute(g):
        blk = g // 4
        for i in (2 * (g % 4), 2 * (g % 4) + 1):
            wait_piece(blk, i)
            if blk == 0:

                @pl.when(z < nz - 1)
                def _():
                    forward_piece(i).start()

            for t in range(16 + 16 * blk + 2 * i, 18 + 16 * blk + 2 * i):
                place(t)
        for pair in range(CHUNK // 2):
            m = CHUNK * g + 2 * pair
            found = jnp.dot(krev[...], w2[(m + 1) * 128 : (m + 17) * 128, :], preferred_element_type=jnp.float32)
            d2s[g, :, pair * 256 : (pair + 1) * 256] = found[128:].astype(jnp.bfloat16)
            d2o[g, :, pair * 256 : (pair + 1) * 256] = found[:128]
        core_copy(g).start()

    def fold(block):
        half = lanes // 2
        return jnp.concatenate([block[:, :half], block[:, half:]], axis=0)

    def after_core(g):
        core_copy(g).wait_recv()
        total = d2o[g] + d2r[g].astype(jnp.float32)
        for d in range(4):
            if order_of(g)[0] == "px":
                block = total[32 * d : 32 * d + 32]
            else:
                block = jnp.concatenate([total[32 * e + 8 * d : 32 * e + 8 * d + 8] for e in range(4)], axis=0)
            if d == 0:
                o1[g] = block
            else:
                s1[g, d - 1] = block.astype(jnp.bfloat16)
        for d in (2, 1, 3):
            first_copy(g, d).start()

    def after_first(g):
        total = o1[g]
        for d in (1, 3, 2):
            first_copy(g, d).wait_recv()
            total = total + r1[g, d - 1].astype(jnp.float32)
        for d in range(4):
            block = fold(total[8 * d : 8 * d + 8])
            if d == 0:
                o2[g] = block
            else:
                s2[g, d - 1] = block.astype(jnp.bfloat16)
        for d in (2, 1, 3):
            second_copy(g, d).start()

    def after_second(g):
        total = o2[g]
        for d in (1, 3, 2):
            second_copy(g, d).wait_recv()
            total = total + r2[g, d - 1].astype(jnp.float32)
        for high in range(2):
            for low in range(CHUNK // 2):
                m = CHUNK * g + high * (CHUNK // 2) + low
                yb[m * 8 : m * 8 + 8, :] = total[high * 8 : high * 8 + 8, low * 128 : (low + 1) * 128]

    def send_z(s):
        for d in range(8):
            rows = yb[pl.ds(s * 128 + d, 16, stride=8), :]
            if d == 0:
                zo[s] = rows
            else:
                zs[s, d - 1] = rows.astype(jnp.bfloat16)
        for d in (4, 3, 5, 2, 6, 1, 7):
            z_copy(s, d).start()

    def finish(s):
        total = zo[s]
        for d in range(1, 8):
            z_copy(s, d).wait_recv()
            total = total + zr[s, d - 1].astype(jnp.float32)
        out_ref[s * 16 : (s + 1) * 16, :] = total.astype(jnp.bfloat16)

    def relay_on(s):
        for owner in (4, 5, 6):

            @pl.when(z == owner - 3)
            def _():
                to_relay(s).wait_recv()
                from_relay(s, owner).start()

    for step in range(chunks + 5):
        if step < chunks:
            compute(step)
        if step == 1:
            relay_on(0)
        if step == 2:
            relay_on(1)
        if 0 <= step - 1 < chunks:
            after_core(step - 1)
        if 0 <= step - 3 < chunks:
            after_first(step - 3)
        if 0 <= step - 5 < chunks:
            after_second(step - 5)
        if step - 5 == chunks // 2 - 1:
            send_z(0)
    send_z(1)
    finish(0)
    finish(1)

    @pl.when(z < nz - 1)
    def _():
        for i in range(8):
            own_piece(i).wait_send()
            forward_piece(i).wait_send()

    for s in range(2):
        for owner in (1, 2, 3, 7):

            @pl.when(z == owner)
            def _():
                arrival_piece(s, owner).wait_send()

        for owner in (4, 5, 6):

            @pl.when(z == owner)
            def _():
                to_relay(s).wait_send()

            @pl.when(z == owner - 3)
            def _():
                from_relay(s, owner).wait_send()

    for g in range(chunks):
        core_copy(g).wait_send()
        for d in range(1, 4):
            first_copy(g, d).wait_send()
            second_copy(g, d).wait_send()
    for s in range(2):
        for d in range(1, 8):
            z_copy(s, d).wait_send()


def per_device(lags, history, arrivals):
    chunks = 32 // CHUNK
    lanes = CHUNK * 128
    bf16, f32 = jnp.bfloat16, jnp.float32
    dma = pltpu.SemaphoreType.DMA
    found = pl.pallas_call(
        kernel,
        out_shape=jax.ShapeDtypeStruct((32, 128), bf16),
        in_specs=[pl.BlockSpec(memory_space=pl.ANY)] * 3,
        out_specs=pl.BlockSpec(memory_space=pltpu.VMEM),
        scratch_shapes=[
            pltpu.VMEM((16, 256, 128), bf16),
            pltpu.VMEM((256, 2048), bf16),
            pltpu.VMEM((48, 128, 128), bf16),
            pltpu.VMEM((48 * 128, 256), bf16),
            pltpu.VMEM((2, 2, 128, 128), bf16),
            pltpu.VMEM((chunks, 128, lanes), bf16),
            pltpu.VMEM((chunks, 128, lanes), f32),
            pltpu.VMEM((chunks, 128, lanes), bf16),
            pltpu.VMEM((chunks, 3, 32, lanes), bf16),
            pltpu.VMEM((chunks, 32, lanes), f32),
            pltpu.VMEM((chunks, 3, 32, lanes), bf16),
            pltpu.VMEM((chunks, 3, 16, lanes // 2), bf16),
            pltpu.VMEM((chunks, 16, lanes // 2), f32),
            pltpu.VMEM((chunks, 3, 16, lanes // 2), bf16),
            pltpu.VMEM((256, 128), f32),
            pltpu.VMEM((2, 7, 16, 128), bf16),
            pltpu.VMEM((2, 16, 128), f32),
            pltpu.VMEM((2, 7, 16, 128), bf16),
            dma((2,)),
            dma((2, 8)),
            dma((8,)),
            dma((8,)),
            dma((2,)),
            dma((2,)),
            dma((2,)),
            dma((chunks,)),
            dma((chunks,)),
            dma((chunks, 3)),
            dma((chunks, 3)),
            dma((chunks, 3)),
            dma((chunks, 3)),
            dma((2, 7)),
            dma((2, 7)),
        ],
        compiler_params=pltpu.CompilerParams(
            collective_id=0, has_side_effects=True, vmem_limit_bytes=48 * 1024 * 1024
        ),
    )(lags, history, arrivals)
    return found.reshape(2, 16, 1, 128)


def solution(mesh):
    split = Mesh(mesh.devices.reshape(mesh.shape["tm"], 4, 4, 2), ("tm", *PAR))
    placed = (P("tm", None, PAR), P("tm", PAR, None), P(None, "tm", PAR, None))
    return jax.shard_map(
        per_device,
        mesh=split,
        in_specs=placed,
        out_specs=P(None, None, ("tm", *PAR), None),
        check_vma=False,
    )
```

```python
import jax
import jax.numpy as jnp
from jax import lax
from jax.experimental import pallas as pl
from jax.experimental.pallas import tpu as pltpu
from jax.sharding import Mesh
from jax.sharding import PartitionSpec as P

PAR = ("px", "py", "pc")
MESH = pl.DeviceIdType.MESH
CHUNKS = [(4 * g, 4) for g in range(7)] + [(28, 2), (30, 2)]
WIDE = 4 * 128
PLAN = (
    ("A", 0), ("P", 0), ("S", 1), ("A", 1), ("Q", 1), ("B", 0), ("R", 0), ("B", 1), ("A", 2), ("B", 2), ("A", 3),
    ("T", 0), ("R", 1), ("C", 0), ("B", 3), ("A", 4), ("C", 1), ("B", 4), ("A", 5), ("C", 2), ("D", 0), ("B", 5),
    ("A", 6), ("C", 3), ("D", 1), ("A", 7), ("B", 6), ("C", 4), ("A", 8), ("B", 7), ("B", 8), ("D", 2), ("D", 3),
    ("Z", 0), ("C", 5), ("C", 6), ("C", 7), ("C", 8), ("D", 4), ("D", 5), ("D", 6), ("D", 7), ("D", 8), ("Z", 1),
    ("E", 0), ("F", 0), ("F", 1), ("E", 1),
)


def kernel(k_hbm, h_hbm, a_hbm, out_ref, kv, krev, w, w2, arr, relay, d2s, d2o, d2r, s1, o1, r1, s2, o2, r2, yb, zs, zo, zr,
           rounds, local_sem, w_recv, own_send, fwd_send, arr_send, relay_recv, relay_send, d2_send, d2_recv,
           s1_send, s1_recv, s2_send, s2_recv, z_send, z_recv):
    z, x, y, c = (lax.axis_index(name) for name in ("tm", "px", "py", "pc"))
    nz, nx, ny, nc = 8, 4, 4, 2
    chunks = len(CHUNKS)
    sizes = {"tm": nz, "px": nx, "py": ny, "pc": nc}
    here = {"tm": z, "px": x, "py": y, "pc": c}

    def ahead(name, by):
        return {name: lax.rem(here[name] + by, sizes[name])}

    copy_k = pltpu.make_async_copy(k_hbm, kv, local_sem.at[0])
    copy_k.start()
    copy_h = pltpu.make_async_copy(h_hbm, w.at[pl.ds(0, 16)], local_sem.at[1])
    copy_h.start()
    copy_a = pltpu.make_async_copy(a_hbm, arr, local_sem.at[2])
    copy_a.start()

    barrier = pltpu.get_barrier_semaphore()
    plane = [("px", 1), ("px", nx - 1), ("py", 1), ("py", ny - 1)]

    def greet(sem, peers):
        for name, by in peers:
            pl.semaphore_signal(sem, inc=1, device_id=ahead(name, by), device_id_type=MESH)

    @pl.when(z > 0)
    def _():
        greet(barrier, [("tm", nz - 1)])

    for by in (1, 2, 3):

        @pl.when(z + by < nz)
        def _():
            greet(barrier, [("tm", by)])

    @pl.when(z == 0)
    def _():
        greet(barrier, [("tm", nz - 1)])

    greet(barrier, plane + [("pc", 1)])
    for count in (1, 2, 3):

        @pl.when(z == count - 1)
        def _():
            pl.semaphore_wait(barrier, 5 + count)

    @pl.when(z >= 3)
    def _():
        pl.semaphore_wait(barrier, 5 + 4)

    def remote(src, dst, send_sem, recv_sem, target):
        return pltpu.make_async_remote_copy(
            src_ref=src, dst_ref=dst, send_sem=send_sem, recv_sem=recv_sem, device_id=target, device_id_type=MESH
        )

    def own_piece(i):
        return remote(
            w.at[pl.ds(2 * i, 2)], w.at[pl.ds(16 + 2 * i, 2)], own_send.at[0], w_recv.at[0, i], ahead("tm", 1)
        )

    def forward_piece(i):
        return remote(
            w.at[pl.ds(16 + 2 * i, 2)], w.at[pl.ds(32 + 2 * i, 2)], fwd_send.at[0], w_recv.at[1, i], ahead("tm", 1)
        )

    def wait_piece(blk, i):
        ref = w.at[pl.ds(16 + 16 * blk + 2 * i, 2)]
        remote(ref, ref, fwd_send.at[0], w_recv.at[blk, i], ahead("tm", 1)).wait_recv()

    def arrival_piece(s, owner):
        return remote(
            arr.at[s], w.at[pl.ds(16 + 16 * s + 2 * owner, 2)], arr_send.at[s], w_recv.at[s, owner], {"tm": 0}
        )

    def to_relay(s):
        return remote(arr.at[s], relay.at[s], arr_send.at[s], relay_recv.at[s], ahead("tm", nz - 3))

    def from_relay(s, owner):
        return remote(
            relay.at[s], w.at[pl.ds(16 + 16 * s + 2 * owner, 2)], relay_send.at[s], w_recv.at[s, owner], {"tm": 0}
        )

    def local_arrival(s):
        return pltpu.make_async_copy(a_hbm.at[s], w.at[pl.ds(16 + 16 * s, 2)], w_recv.at[s, 0])

    @pl.when(z == 0)
    def _():
        for s in range(2):
            local_arrival(s).start()

    def send_direct(s):
        for owner in (1, 2, 3, 7):

            @pl.when(z == owner)
            def _():
                arrival_piece(s, owner).start()

    def send_to_relay(s):
        @pl.when((z >= 4) & (z <= 6))
        def _():
            to_relay(s).start()

    greet(rounds.at[0], plane)
    copy_h.wait()

    @pl.when(z < nz - 1)
    def _():
        for i in range(8):
            own_piece(i).start()

    copy_a.wait()
    send_direct(0)
    send_to_relay(0)

    row = lax.broadcasted_iota(jnp.int32, (256, 256), 0)
    col = lax.broadcasted_iota(jnp.int32, (256, 256), 1)
    core_of = (c + (row >> 7)) & 1
    x_of = (x + (row >> 5)) & 3
    y_of = (y + (row >> 3)) & 3
    z_of = (z + row) & 7
    sensor = z_of * 32 + x_of * 8 + y_of * 2 + core_of
    order = jnp.where(sensor == col, 1.0, 0.0).astype(jnp.bfloat16)
    copy_k.wait()
    for lag in range(16):
        moved = jnp.dot(order, kv[lag], preferred_element_type=jnp.float32)
        krev[:, (15 - lag) * 128 : (16 - lag) * 128] = moved.astype(jnp.bfloat16)

    def place(t):
        block = w[t]
        w2[t * 128 : (t + 1) * 128, 0:128] = block
        if t > 0:
            w2[(t - 1) * 128 : t * 128, 128:256] = block

    for t in range(16):
        place(t)

    def order_of(g):
        return ("px", "py") if g % 2 == 0 else ("py", "px")

    def lanes_of(g):
        return CHUNKS[g][1] * 128

    def core_copy(g):
        lanes = pl.ds(0, lanes_of(g))
        return remote(d2s.at[g, :, lanes], d2r.at[g, :, lanes], d2_send.at[0], d2_recv.at[g], ahead("pc", 1))

    def first_copy(g, d):
        lanes = pl.ds(0, lanes_of(g))
        return remote(
            s1.at[g, d - 1, :, lanes],
            r1.at[g, d - 1, :, lanes],
            s1_send.at[0],
            s1_recv.at[g],
            ahead(order_of(g)[0], d),
        )

    def second_copy(g, d):
        lanes = pl.ds(0, lanes_of(g) // 2)
        return remote(
            s2.at[g, d - 1, :, lanes],
            r2.at[g, d - 1, :, lanes],
            s2_send.at[0],
            s2_recv.at[g],
            ahead(order_of(g)[1], d),
        )

    def z_copy(s, d):
        return remote(zs.at[s, d - 1], zr.at[s, d - 1], z_send.at[0], z_recv.at[s], ahead("tm", d))

    def landed(ref, sem):
        remote(ref, ref, z_send.at[0], sem, ahead("tm", 1)).wait_recv()

    def left(ref, sem):
        remote(ref, ref, sem, z_recv.at[0], ahead("tm", 1)).wait_send()

    def compute(g):
        first, size = CHUNKS[g]
        blk = first // 16

        def part(m, low, high, rows=slice(0, 256)):
            return jnp.dot(
                krev[rows, low * 128 : high * 128],
                w2[(m + 1 + low) * 128 : (m + 1 + high) * 128, :],
                preferred_element_type=jnp.float32,
            )

        mine, other = slice(0, 128), slice(128, 256)
        if size == 2:
            early_other, early_mine = part(first, 0, 14, other), part(first, 0, 14, mine)
        for i in range((first % 16) // 2, (first % 16 + size) // 2):
            wait_piece(blk, i)
            if blk == 0:

                @pl.when(z < nz - 1)
                def _():
                    forward_piece(i).start()

            for t in range(16 + 16 * blk + 2 * i, 18 + 16 * blk + 2 * i):
                place(t)
        if size == 2:
            d2s[g, :, :256] = (early_other + part(first, 14, 16, other)).astype(jnp.bfloat16)
            core_copy(g).start()
            d2o[g, :, :256] = early_mine + part(first, 14, 16, mine)
            return
        for pair in range(size // 2):
            m = first + 2 * pair
            found = part(m, 0, 16)
            d2s[g, :, pair * 256 : (pair + 1) * 256] = found[128:].astype(jnp.bfloat16)
            d2o[g, :, pair * 256 : (pair + 1) * 256] = found[:128]
        core_copy(g).start()

    def fold(block):
        half = block.shape[1] // 2
        return jnp.concatenate([block[:, :half], block[:, half:]], axis=0)

    def after_core(g):
        lanes = lanes_of(g)
        core_copy(g).wait_recv()
        total = d2o[g, :, :lanes] + d2r[g, :, :lanes].astype(jnp.float32)
        for d in range(4):
            if order_of(g)[0] == "px":
                block = total[32 * d : 32 * d + 32]
            else:
                block = jnp.concatenate([total[32 * e + 8 * d : 32 * e + 8 * d + 8] for e in range(4)], axis=0)
            if d == 0:
                o1[g, :, :lanes] = block
            else:
                s1[g, d - 1, :, :lanes] = block.astype(jnp.bfloat16)
        for d in (2, 1, 3):
            first_copy(g, d).start()

    def after_first(g):
        lanes = lanes_of(g)
        total = o1[g, :, :lanes]
        landed(r1.at[g, :, :, pl.ds(0, lanes)], s1_recv.at[g])
        for d in (1, 3, 2):
            total = total + r1[g, d - 1, :, :lanes].astype(jnp.float32)
        for d in range(4):
            block = fold(total[8 * d : 8 * d + 8])
            if d == 0:
                o2[g, :, : lanes // 2] = block
            else:
                s2[g, d - 1, :, : lanes // 2] = block.astype(jnp.bfloat16)
        for d in (2, 1, 3):
            second_copy(g, d).start()

    def after_second(g):
        first, size = CHUNKS[g]
        lanes = lanes_of(g) // 2
        total = o2[g, :, :lanes]
        landed(r2.at[g, :, :, pl.ds(0, lanes)], s2_recv.at[g])
        for d in (1, 3, 2):
            total = total + r2[g, d - 1, :, :lanes].astype(jnp.float32)
        for high in range(2):
            for low in range(size // 2):
                m = first + high * (size // 2) + low
                yb[m * 8 : m * 8 + 8, :] = total[high * 8 : high * 8 + 8, low * 128 : (low + 1) * 128]

    def meet_plane(_):
        pl.semaphore_wait(rounds.at[0], len(plane))

    def tell_all(_):
        @pl.when(z == 0)
        def _():
            greet(rounds.at[1], [("tm", by) for by in range(1, nz)])

    def send_z(s):
        if s == 0:

            @pl.when(z > 0)
            def _():
                pl.semaphore_wait(rounds.at[1], 1)

        for d in range(8):
            rows = yb[pl.ds(s * 128 + d, 16, stride=8), :]
            if d == 0:
                zo[s] = rows
            else:
                zs[s, d - 1] = rows.astype(jnp.bfloat16)
        for d in (4, 3, 5, 2, 6, 1, 7):
            z_copy(s, d).start()

    def finish(s):
        total = zo[s]
        landed(zr.at[s], z_recv.at[s])
        for d in range(1, 8):
            total = total + zr[s, d - 1].astype(jnp.float32)
        out_ref[s * 16 : (s + 1) * 16, :] = total.astype(jnp.bfloat16)

    def relay_on(s):
        for owner in (4, 5, 6):

            @pl.when(z == owner - 3)
            def _():
                to_relay(s).wait_recv()
                from_relay(s, owner).start()

    def end_sends(part):
        if part == 1:
            left(zs, z_send.at[0])
            return

        @pl.when(z < nz - 1)
        def _():
            left(w.at[pl.ds(0, 16)], own_send.at[0])
            left(w.at[pl.ds(16, 16)], fwd_send.at[0])

        for s in range(2):
            for owner in (1, 2, 3, 7):

                @pl.when(z == owner)
                def _():
                    arrival_piece(s, owner).wait_send()

            for owner in (4, 5, 6):

                @pl.when(z == owner)
                def _():
                    to_relay(s).wait_send()

                @pl.when(z == owner - 3)
                def _():
                    from_relay(s, owner).wait_send()

        left(d2s.at[pl.ds(0, chunks - 1)], d2_send.at[0])
        left(s1.at[pl.ds(0, chunks - 1)], s1_send.at[0])
        left(s2.at[pl.ds(0, chunks - 1)], s2_send.at[0])

    stages = {"A": compute, "B": after_core, "C": after_first, "D": after_second, "R": relay_on, "Z": send_z, "F": finish, "S": send_direct, "Q": send_to_relay}
    stages |= {"P": meet_plane, "T": tell_all, "E": end_sends}
    for stage, number in PLAN:
        stages[stage](number)


def per_device(lags, history, arrivals):
    chunks, lanes = len(CHUNKS), WIDE
    bf16, f32 = jnp.bfloat16, jnp.float32
    dma = pltpu.SemaphoreType.DMA
    found = pl.pallas_call(
        kernel,
        out_shape=jax.ShapeDtypeStruct((32, 128), bf16),
        in_specs=[pl.BlockSpec(memory_space=pltpu.HBM)] * 3,
        out_specs=pl.BlockSpec(memory_space=pltpu.VMEM),
        scratch_shapes=[
            pltpu.VMEM((16, 256, 128), bf16),
            pltpu.VMEM((256, 2048), bf16),
            pltpu.VMEM((48, 128, 128), bf16),
            pltpu.VMEM((48 * 128, 256), bf16),
            pltpu.VMEM((2, 2, 128, 128), bf16),
            pltpu.VMEM((2, 2, 128, 128), bf16),
            pltpu.VMEM((chunks, 128, lanes), bf16),
            pltpu.VMEM((chunks, 128, lanes), f32),
            pltpu.VMEM((chunks, 128, lanes), bf16),
            pltpu.VMEM((chunks, 3, 32, lanes), bf16),
            pltpu.VMEM((chunks, 32, lanes), f32),
            pltpu.VMEM((chunks, 3, 32, lanes), bf16),
            pltpu.VMEM((chunks, 3, 16, lanes // 2), bf16),
            pltpu.VMEM((chunks, 16, lanes // 2), f32),
            pltpu.VMEM((chunks, 3, 16, lanes // 2), bf16),
            pltpu.VMEM((256, 128), f32),
            pltpu.VMEM((2, 7, 16, 128), bf16),
            pltpu.VMEM((2, 16, 128), f32),
            pltpu.VMEM((2, 7, 16, 128), bf16),
            pltpu.SemaphoreType.REGULAR((2,)),
            dma((3,)),
            dma((2, 8)),
            dma((1,)),
            dma((1,)),
            dma((2,)),
            dma((2,)),
            dma((2,)),
            dma((1,)),
            dma((chunks,)),
            dma((1,)),
            dma((chunks,)),
            dma((1,)),
            dma((chunks,)),
            dma((1,)),
            dma((2,)),
        ],
        compiler_params=pltpu.CompilerParams(
            collective_id=0, has_side_effects=True, vmem_limit_bytes=55168 * 1024
        ),
    )(lags, history, arrivals)
    return found.reshape(2, 16, 1, 128)


def solution(mesh):
    split = Mesh(mesh.devices.reshape(mesh.shape["tm"], 4, 4, 2), ("tm", *PAR))
    placed = (P("tm", None, PAR), P("tm", PAR, None), P(None, "tm", PAR, None))
    return jax.shard_map(
        per_device,
        mesh=split,
        in_specs=placed,
        out_specs=P(None, None, ("tm", *PAR), None),
        check_vma=False,
    )
```

```python
import jax
import jax.numpy as jnp
from jax import lax
from jax.experimental import pallas as pl
from jax.experimental.pallas import tpu as pltpu
from jax.sharding import Mesh
from jax.sharding import PartitionSpec as P

PAR = ("px", "py", "pc")
MESH = pl.DeviceIdType.MESH
CHUNKS = [(4 * g, 4) for g in range(6)] + [(24, 2), (26, 2), (28, 2), (30, 2)]
WHOLE = 8
PIECES = (8, 8, 7, 7, 6, 6, 5, 5)
LAGS = tuple(16 - 2 * n for n in PIECES)
MOST = max(LAGS)
WIDE = 4 * 128
PLAN = (
    ("A", 0), ("P", 0), ("S", 1), ("Q", 1), ("A", 1), ("B", 0), ("R", 0), ("B", 1), ("A", 2), ("B", 2), ("A", 3),
    ("C", 0), ("B", 3), ("R", 1), ("A", 4), ("C", 1), ("V", 6), ("V", 7), ("V", 8), ("V", 9), ("B", 4), ("K", 0),
    ("C", 2), ("D", 0), ("A", 5), ("U", 6), ("U", 7), ("U", 8), ("U", 9), ("C", 3), ("A", 6), ("B", 5), ("A", 7),
    ("A", 8), ("B", 6), ("A", 9), ("B", 7), ("B", 8), ("B", 9), ("D", 1), ("D", 2), ("C", 4), ("D", 3), ("Z", 0),
    ("C", 6), ("C", 5), ("C", 8), ("C", 7), ("C", 9), ("D", 4), ("D", 5), ("D", 6), ("D", 7), ("D", 8), ("D", 9),
    ("Z", 1), ("E", 0), ("F", 0), ("F", 1), ("E", 1),
)
LAST = (
    ("A", 0), ("P", 0), ("S", 1), ("A", 1), ("B", 0), ("B", 1), ("A", 2), ("B", 2), ("A", 3), ("C", 0), ("B", 3),
    ("A", 4), ("C", 1), ("V", 6), ("V", 7), ("V", 8), ("V", 9), ("B", 4), ("C", 2), ("D", 0), ("A", 5), ("C", 3),
    ("N", 6), ("B", 5), ("N", 7), ("N", 8), ("B", 6), ("N", 9), ("B", 7), ("B", 8), ("B", 9), ("D", 1), ("D", 2),
    ("C", 4), ("D", 3), ("Z", 0), ("C", 6), ("C", 5), ("C", 8), ("C", 7), ("C", 9), ("D", 4), ("D", 5), ("D", 6),
    ("D", 7), ("D", 8), ("D", 9), ("Z", 1), ("E", 0), ("F", 0), ("F", 1), ("E", 1),
)
FIRST = (
    ("A", 0), ("P", 0), ("A", 1), ("B", 0), ("B", 1), ("C", 0), ("C", 1), ("A", 2), ("A", 3), ("T", 0), ("B", 2),
    ("A", 4), ("B", 3), ("V", 6), ("V", 7), ("V", 8), ("V", 9), ("B", 4), ("K", 0), ("A", 5), ("U", 6), ("U", 7),
    ("U", 8), ("U", 9), ("B", 5), ("D", 0), ("D", 1), ("A", 6), ("A", 7), ("C", 2), ("A", 8), ("B", 6), ("A", 9),
    ("B", 7), ("B", 8), ("B", 9), ("C", 3), ("C", 4), ("C", 6), ("C", 5), ("D", 2), ("D", 3), ("Z", 0), ("C", 8),
    ("C", 7), ("C", 9), ("D", 4), ("D", 5), ("D", 6), ("D", 7), ("D", 8), ("D", 9), ("Z", 1), ("E", 0), ("F", 0),
    ("F", 1), ("E", 1),
)


def kernel(k_hbm, h_hbm, a_hbm, out_ref, kv, kx, krev, kxrev, orders, acc, v2, w, w2, arr, relay, d2s, d2o, d2r, s1, o1, r1, s2, o2, r2, yb, zs, zo, zr,
           rounds, local_sem, w_recv, own_send, fwd_send, arr_send, relay_recv, relay_send, kx_send, kx_recv, d2_send, d2_recv,
           s1_send, s1_recv, s2_send, s2_recv, z_send, z_recv):
    z, x, y, c = (lax.axis_index(name) for name in ("tm", "px", "py", "pc"))
    nz, nx, ny, nc = 8, 4, 4, 2
    chunks = len(CHUNKS)
    sizes = {"tm": nz, "px": nx, "py": ny, "pc": nc}
    here = {"tm": z, "px": x, "py": y, "pc": c}

    def ahead(name, by):
        return {name: lax.rem(here[name] + by, sizes[name])}

    copy_k = pltpu.make_async_copy(k_hbm, kv, local_sem.at[0])
    copy_k.start()
    copy_h = pltpu.make_async_copy(h_hbm, w.at[pl.ds(0, 16)], local_sem.at[1])
    copy_h.start()
    copy_a = pltpu.make_async_copy(a_hbm, arr, local_sem.at[2])
    copy_a.start()

    kx[...] = jnp.zeros_like(kx)
    w[48 - MOST :] = jnp.zeros((MOST, 128, 128), jnp.bfloat16)
    v2[...] = jnp.zeros_like(v2)

    barrier = pltpu.get_barrier_semaphore()
    plane = [("px", 1), ("px", nx - 1), ("py", 1), ("py", ny - 1)]

    def greet(sem, peers):
        for name, by in peers:
            pl.semaphore_signal(sem, inc=1, device_id=ahead(name, by), device_id_type=MESH)

    @pl.when(z > 0)
    def _():
        greet(barrier, [("tm", nz - 1)])

    for by in (1, 2, 3):

        @pl.when(z + by < nz)
        def _():
            greet(barrier, [("tm", by)])

    @pl.when(z == 0)
    def _():
        greet(barrier, [("tm", nz - 1)])

    greet(barrier, plane + [("pc", 1)])
    for count in (1, 2, 3):

        @pl.when(z == count - 1)
        def _():
            pl.semaphore_wait(barrier, 5 + count)

    @pl.when(z >= 3)
    def _():
        pl.semaphore_wait(barrier, 5 + 4)

    def remote(src, dst, send_sem, recv_sem, target):
        return pltpu.make_async_remote_copy(
            src_ref=src, dst_ref=dst, send_sem=send_sem, recv_sem=recv_sem, device_id=target, device_id_type=MESH
        )

    def own_piece(i):
        return remote(
            w.at[pl.ds(2 * i, 2)], w.at[pl.ds(16 + 2 * i, 2)], own_send.at[0], w_recv.at[0, i], ahead("tm", 1)
        )

    def forward_piece(i):
        return remote(
            w.at[pl.ds(16 + 2 * i, 2)], w.at[pl.ds(32 + 2 * i, 2)], fwd_send.at[0], w_recv.at[1, i], ahead("tm", 1)
        )

    def wait_piece(blk, i):
        ref = w.at[pl.ds(16 + 16 * blk + 2 * i, 2)]
        remote(ref, ref, fwd_send.at[0], w_recv.at[blk, i], ahead("tm", 1)).wait_recv()

    def arrival_piece(s, owner):
        return remote(
            arr.at[s], w.at[pl.ds(16 + 16 * s + 2 * owner, 2)], arr_send.at[s], w_recv.at[s, owner], {"tm": 0}
        )

    def to_relay(s):
        return remote(arr.at[s], relay.at[s], arr_send.at[s], relay_recv.at[s], ahead("tm", nz - 3))

    def from_relay(s, owner):
        return remote(
            relay.at[s], w.at[pl.ds(16 + 16 * s + 2 * owner, 2)], relay_send.at[s], w_recv.at[s, owner], {"tm": 0}
        )

    def local_arrival(s):
        return pltpu.make_async_copy(a_hbm.at[s], w.at[pl.ds(16 + 16 * s, 2)], w_recv.at[s, 0])

    @pl.when(z == 0)
    def _():
        for s in range(2):
            local_arrival(s).start()

    def send_direct(s):
        for owner in (1, 2, 3, 7):

            @pl.when(z == owner)
            def _():
                arrival_piece(s, owner).start()

    def send_to_relay(s):
        @pl.when((z >= 4) & (z <= 6))
        def _():
            to_relay(s).start()

    greet(rounds.at[0], plane)
    copy_h.wait()

    @pl.when(z < nz - 1)
    def _():
        for i in range(8):
            own_piece(i).start()

    copy_a.wait()
    send_direct(0)
    send_to_relay(0)

    row = lax.broadcasted_iota(jnp.int32, (256, 256), 0)
    col = lax.broadcasted_iota(jnp.int32, (256, 256), 1)
    core_of = (c + (row >> 7)) & 1
    x_of = (x + (row >> 5)) & 3
    y_of = (y + (row >> 3)) & 3
    z_of = (z + row) & 7
    sensor = z_of * 32 + x_of * 8 + y_of * 2 + core_of
    orders[...] = jnp.where(sensor == col, 1.0, 0.0).astype(jnp.bfloat16)
    copy_k.wait()

    def lags_down(owner):
        lags = pl.ds(0, LAGS[owner])
        return remote(kv.at[lags], kx.at[lags], kx_send.at[0], kx_recv.at[0], {"tm": owner - 1})

    for owner in range(1, nz):
        if LAGS[owner]:

            @pl.when(z == owner)
            def _():
                lags_down(owner).start()

    for lag in range(16):
        moved = jnp.dot(orders[...], kv[lag], preferred_element_type=jnp.float32)
        krev[:, (15 - lag) * 128 : (16 - lag) * 128] = moved.astype(jnp.bfloat16)

    def place(t):
        block = w[t]
        w2[t * 128 : (t + 1) * 128, 0:128] = block
        if t > 0:
            w2[(t - 1) * 128 : t * 128, 128:256] = block

    for t in range(16):
        place(t)

    def order_of(g):
        return ("px", "py") if g % 2 == 0 else ("py", "px")

    def lanes_of(g):
        return CHUNKS[g][1] * 128

    def core_copy(g):
        lanes = pl.ds(0, lanes_of(g))
        return remote(d2s.at[g, :, lanes], d2r.at[g, :, lanes], d2_send.at[0], d2_recv.at[g], ahead("pc", 1))

    def first_copy(g, d):
        lanes = pl.ds(0, lanes_of(g))
        return remote(
            s1.at[g, d - 1, :, lanes],
            r1.at[g, d - 1, :, lanes],
            s1_send.at[0],
            s1_recv.at[g],
            ahead(order_of(g)[0], d),
        )

    def second_copy(g, d):
        lanes = pl.ds(0, lanes_of(g) // 2)
        return remote(
            s2.at[g, d - 1, :, lanes],
            r2.at[g, d - 1, :, lanes],
            s2_send.at[0],
            s2_recv.at[g],
            ahead(order_of(g)[1], d),
        )

    def z_copy(s, d):
        return remote(zs.at[s, d - 1], zr.at[s, d - 1], z_send.at[0], z_recv.at[s], ahead("tm", d))

    def landed(ref, sem):
        remote(ref, ref, z_send.at[0], sem, ahead("tm", 1)).wait_recv()

    def left(ref, sem):
        remote(ref, ref, sem, z_recv.at[0], ahead("tm", 1)).wait_send()

    def last_with(i):
        return max(at for at in range(nz) if PIECES[at] > i)

    def part(m, low, high, rows=slice(0, 256)):
        return jnp.dot(
            krev[rows, low * 128 : high * 128],
            w2[(m + 1 + low) * 128 : (m + 1 + high) * 128, :],
            preferred_element_type=jnp.float32,
        )

    def early(g):
        m = CHUNKS[g][0]
        acc[g] = part(m, 0, 34 - m)

    def later(g):
        m = CHUNKS[g][0]
        acc[g] = acc[g] + part(m, 34 - m, 38 - m)

    def given_lags(_):
        for owner in range(1, nz):
            if LAGS[owner]:

                @pl.when(z == owner - 1)
                def _():
                    lags_down(owner).wait_recv()

                    for u in range(LAGS[owner]):
                        at = 2 * MOST - LAGS[owner] - 1 + u
                        block = w[32 - LAGS[owner] + u]
                        if at < 2 * MOST:
                            v2[at * 128 : (at + 1) * 128, 0:128] = block
                        v2[(at - 1) * 128 : at * 128, 128:256] = block

        for lag in range(MOST):
            moved = jnp.dot(orders[...], kx[lag], preferred_element_type=jnp.float32)
            kxrev[:, (MOST - 1 - lag) * 128 : (MOST - lag) * 128] = moved.astype(jnp.bfloat16)
        for g, (m, size) in enumerate(CHUNKS):
            if m + 2 > 32 - MOST:
                at = m - (32 - MOST)
                acc[g] = acc[g] + jnp.dot(
                    kxrev[...], v2[at * 128 : (at + MOST) * 128, :], preferred_element_type=jnp.float32
                )

    def compute(g, since=38):
        first, size = CHUNKS[g]
        blk = first // 16
        for i in range((first % 16) // 2, (first % 16 + size) // 2):
            if blk == 0:
                wait_piece(0, i)

                @pl.when(z < last_with(i))
                def _():
                    forward_piece(i).start()

            elif last_with(i) == nz - 1:
                wait_piece(1, i)
            else:

                @pl.when(z <= last_with(i))
                def _():
                    wait_piece(1, i)

            for t in range(16 + 16 * blk + 2 * i, 18 + 16 * blk + 2 * i):
                place(t)
        if size == 2:
            mine, other = slice(0, 128), slice(128, 256)
            d2s[g, :, :256] = (acc[g, 128:] + part(first, since - first, 16, other)).astype(jnp.bfloat16)
            core_copy(g).start()
            d2o[g, :, :256] = acc[g, :128] + part(first, since - first, 16, mine)
            return
        for pair in range(size // 2):
            found = part(first + 2 * pair, 0, 16)
            d2s[g, :, pair * 256 : (pair + 1) * 256] = found[128:].astype(jnp.bfloat16)
            d2o[g, :, pair * 256 : (pair + 1) * 256] = found[:128]
        core_copy(g).start()

    def fold(block):
        half = block.shape[1] // 2
        return jnp.concatenate([block[:, :half], block[:, half:]], axis=0)

    def after_core(g):
        lanes = lanes_of(g)
        core_copy(g).wait_recv()
        total = d2o[g, :, :lanes] + d2r[g, :, :lanes].astype(jnp.float32)
        for d in range(4):
            if order_of(g)[0] == "px":
                block = total[32 * d : 32 * d + 32]
            else:
                block = jnp.concatenate([total[32 * e + 8 * d : 32 * e + 8 * d + 8] for e in range(4)], axis=0)
            if d == 0:
                o1[g, :, :lanes] = block
            else:
                s1[g, d - 1, :, :lanes] = block.astype(jnp.bfloat16)
        for d in (2, 1, 3):
            first_copy(g, d).start()

    def after_first(g):
        lanes = lanes_of(g)
        total = o1[g, :, :lanes]
        landed(r1.at[g, :, :, pl.ds(0, lanes)], s1_recv.at[g])
        for d in (1, 3, 2):
            total = total + r1[g, d - 1, :, :lanes].astype(jnp.float32)
        for d in range(4):
            block = fold(total[8 * d : 8 * d + 8])
            if d == 0:
                o2[g, :, : lanes // 2] = block
            else:
                s2[g, d - 1, :, : lanes // 2] = block.astype(jnp.bfloat16)
        for d in (2, 1, 3):
            second_copy(g, d).start()

    def after_second(g):
        first, size = CHUNKS[g]
        lanes = lanes_of(g) // 2
        total = o2[g, :, :lanes]
        landed(r2.at[g, :, :, pl.ds(0, lanes)], s2_recv.at[g])
        for d in (1, 3, 2):
            total = total + r2[g, d - 1, :, :lanes].astype(jnp.float32)
        for high in range(2):
            for low in range(size // 2):
                m = first + high * (size // 2) + low
                yb[m * 8 : m * 8 + 8, :] = total[high * 8 : high * 8 + 8, low * 128 : (low + 1) * 128]

    def meet_plane(_):
        pl.semaphore_wait(rounds.at[0], len(plane))

    def tell_all(_):
        @pl.when(z == 0)
        def _():
            greet(rounds.at[1], [("tm", by) for by in range(1, nz)])

    def send_z(s):
        if s == 0:

            @pl.when(z > 0)
            def _():
                pl.semaphore_wait(rounds.at[1], 1)

        for d in range(8):
            rows = yb[pl.ds(s * 128 + d, 16, stride=8), :]
            if d == 0:
                zo[s] = rows
            else:
                zs[s, d - 1] = rows.astype(jnp.bfloat16)
        for d in (4, 3, 5, 2, 6, 1, 7):
            z_copy(s, d).start()

    def finish(s):
        total = zo[s]
        landed(zr.at[s], z_recv.at[s])
        for d in range(1, 8):
            total = total + zr[s, d - 1].astype(jnp.float32)
        out_ref[s * 16 : (s + 1) * 16, :] = total.astype(jnp.bfloat16)

    def relay_on(s):
        for owner in (4, 5, 6):

            @pl.when(z == owner - 3)
            def _():
                to_relay(s).wait_recv()
                from_relay(s, owner).start()

    def end_sends(part):
        if part == 1:
            left(zs, z_send.at[0])
            return

        for at in range(nz - 1):

            @pl.when(z == at)
            def _():
                left(w.at[pl.ds(0, 16)], own_send.at[0])
                left(w.at[pl.ds(16, 2 * PIECES[at + 1])], fwd_send.at[0])

        for owner in range(1, nz):
            if LAGS[owner]:

                @pl.when(z == owner)
                def _():
                    lags_down(owner).wait_send()

        for s in range(2):
            for owner in (1, 2, 3, 7):

                @pl.when(z == owner)
                def _():
                    arrival_piece(s, owner).wait_send()

            for owner in (4, 5, 6):

                @pl.when(z == owner)
                def _():
                    to_relay(s).wait_send()

                @pl.when(z == owner - 3)
                def _():
                    from_relay(s, owner).wait_send()

        left(d2s.at[pl.ds(0, WHOLE)], d2_send.at[0])
        left(s1.at[pl.ds(0, WHOLE)], s1_send.at[0])
        left(s2.at[pl.ds(0, WHOLE)], s2_send.at[0])

    inner = (z > 0) & (z < nz - 1)
    stages = {"A": compute, "B": after_core, "C": after_first, "D": after_second, "R": relay_on, "Z": send_z, "F": finish, "S": send_direct}
    stages |= {"P": meet_plane, "T": tell_all, "E": end_sends, "K": given_lags, "V": early, "U": later, "Q": send_to_relay, "N": lambda g: compute(g, 34)}
    for here_now, plan in ((inner, PLAN), (z == 0, FIRST), (z == nz - 1, LAST)):

        @pl.when(here_now)
        def _():
            for stage, number in plan:
                stages[stage](number)


def per_device(lags, history, arrivals):
    chunks, lanes = len(CHUNKS), WIDE
    bf16, f32 = jnp.bfloat16, jnp.float32
    dma = pltpu.SemaphoreType.DMA
    found = pl.pallas_call(
        kernel,
        out_shape=jax.ShapeDtypeStruct((32, 128), bf16),
        in_specs=[pl.BlockSpec(memory_space=pltpu.HBM)] * 3,
        out_specs=pl.BlockSpec(memory_space=pltpu.VMEM),
        scratch_shapes=[
            pltpu.VMEM((16, 256, 128), bf16),
            pltpu.VMEM((MOST, 256, 128), bf16),
            pltpu.VMEM((256, 2048), bf16),
            pltpu.VMEM((256, MOST * 128), bf16),
            pltpu.VMEM((256, 256), bf16),
            pltpu.VMEM((chunks, 256, 256), f32),
            pltpu.VMEM((2 * MOST * 128, 256), bf16),
            pltpu.VMEM((48, 128, 128), bf16),
            pltpu.VMEM((48 * 128, 256), bf16),
            pltpu.VMEM((2, 2, 128, 128), bf16),
            pltpu.VMEM((2, 2, 128, 128), bf16),
            pltpu.VMEM((chunks, 128, lanes), bf16),
            pltpu.VMEM((chunks, 128, lanes), f32),
            pltpu.VMEM((chunks, 128, lanes), bf16),
            pltpu.VMEM((chunks, 3, 32, lanes), bf16),
            pltpu.VMEM((chunks, 32, lanes), f32),
            pltpu.VMEM((chunks, 3, 32, lanes), bf16),
            pltpu.VMEM((chunks, 3, 16, lanes // 2), bf16),
            pltpu.VMEM((chunks, 16, lanes // 2), f32),
            pltpu.VMEM((chunks, 3, 16, lanes // 2), bf16),
            pltpu.VMEM((256, 128), f32),
            pltpu.VMEM((2, 7, 16, 128), bf16),
            pltpu.VMEM((2, 16, 128), f32),
            pltpu.VMEM((2, 7, 16, 128), bf16),
            pltpu.SemaphoreType.REGULAR((2,)),
            dma((3,)),
            dma((2, 8)),
            dma((1,)),
            dma((1,)),
            dma((2,)),
            dma((2,)),
            dma((2,)),
            dma((1,)),
            dma((1,)),
            dma((1,)),
            dma((chunks,)),
            dma((1,)),
            dma((chunks,)),
            dma((1,)),
            dma((chunks,)),
            dma((1,)),
            dma((2,)),
        ],
        compiler_params=pltpu.CompilerParams(
            collective_id=0, has_side_effects=True, vmem_limit_bytes=55168 * 1024
        ),
    )(lags, history, arrivals)
    return found.reshape(2, 16, 1, 128)


def solution(mesh):
    split = Mesh(mesh.devices.reshape(mesh.shape["tm"], 4, 4, 2), ("tm", *PAR))
    placed = (P("tm", None, PAR), P("tm", PAR, None), P(None, "tm", PAR, None))
    return jax.shard_map(
        per_device,
        mesh=split,
        in_specs=placed,
        out_specs=P(None, None, ("tm", *PAR), None),
        check_vma=False,
    )
```
